32 devices in a mesh: dp: 4 (over y, x), vocab: 8 (over z, core).
Axes of the slice: x: 2, y: 2, z: 4, core: 2. Of those that a mesh axis runs over, the one named last changes fastest.
Arguments:
- hidden_states: bfloat16 [512, 3584], P('dp'), may hold values from -60 to 60
- unembed: bfloat16 [3584, 32768], P(None, ('dp', 'vocab')), may hold values from -0.3125 to 0.3125
- temp_code: int32 [512], P('dp'), may hold values from 20 to 200
- minp_code: int32 [512], P('dp'), may hold values from 1 to 30
Outputs:
- log_norm: float32 [512], P('dp')
- kept_mass: float32 [512], P('dp')
- kept_count: float32 [512], P('dp')
The draws below stay inside these ranges and needn't reach their ends.
All inputs are finite; a program needn't handle non-finite values.
Results may differ from the reference program's by a relative error of at most 0.0003.
Values may be sent and summed in bfloat16 or wider, within the bound.
A program may use at most 64 MiB of HBM per device.

```python
from functools import partial
import jax
import jax.numpy as jnp
from jax import lax

D = 3584
ROWS_DEV = 128
VOCAB = 32768
BATCH = 512
N_DP = 4


def draw_hidden_states(key, part):
    base_key = jax.random.fold_in(key, 0)
    values = jnp.clip(jax.random.normal(base_key, (BATCH, D), jnp.float32), -6.0, 6.0)
    return values.astype(jnp.bfloat16)


def set_ends(values, stream_key, least, high):
    place = [jax.random.randint(jax.random.fold_in(stream_key, axis), (), 0, length) for axis, length in enumerate(values.shape)]
    widest = values.shape.index(max(values.shape))
    next_to = place[:widest] + [(place[widest] + 1) % values.shape[widest]] + place[widest + 1:]
    return values.at[tuple(place)].set(least).at[tuple(next_to)].set(high)


def block_levels(rng, extent, cuts, low, high):
    level, own = 1.0, jax.random.fold_in(rng, 6)
    for axis_at, parts in cuts:
        draws = jnp.exp(jax.random.uniform(jax.random.fold_in(own, axis_at), (parts,), jnp.float32, low / len(cuts), high / len(cuts)))
        level = level * jnp.repeat(draws, extent[axis_at] // parts).reshape([-1 if axis == axis_at else 1 for axis in range(len(extent))])
    return level


def scatter_about(key, extent, width, reach, shards=(), held_as=jnp.bfloat16):
    array = width * jax.random.normal(key, extent, jnp.float32)
    if shards:
        array = array * block_levels(key, extent, shards, -0.22, 0.18)
    return jnp.clip(array, -reach, reach).astype(held_as)


def setup_inputs(seed: int = 0) -> dict:
    splits = jax.random.split(jax.random.key(seed), 5)
    hidden_states = draw_hidden_states(jax.random.fold_in(splits[4], 71), 0)
    unembed = scatter_about(splits[1], (D, VOCAB), (D // 9) ** -0.5, 0.3125, ((1, 32),))
    temp_code = set_ends(jax.random.randint(splits[2], (BATCH,), 20, 201), jax.random.fold_in(splits[2], 1), 20, 200).astype(jnp.int32)
    minp_code = set_ends(jax.random.randint(splits[3], (BATCH,), 1, 31), jax.random.fold_in(splits[3], 1), 1, 30).astype(jnp.int32)
    return dict(hidden_states=hidden_states, unembed=unembed, temp_code=temp_code, minp_code=minp_code)


def block_stats(unembed, argument_group):
    latent_state_tile, softness_tile, floor_ratio_tile = argument_group
    raw_token_energy = jnp.dot(latent_state_tile, unembed, preferred_element_type=jnp.float32)
    draw_softness_factor = softness_tile.astype(jnp.float32) * 0.01
    min_prob = floor_ratio_tile.astype(jnp.float32) * 0.01
    divided_token_energy = raw_token_energy / draw_softness_factor[:, None]
    top_score = jnp.max(divided_token_energy, axis=1)
    exponent_values = jnp.exp(divided_token_energy - top_score[:, None])
    total = jnp.sum(exponent_values, axis=1)
    ramp = jnp.clip(1.0 + divided_token_energy - top_score[:, None] - jnp.log(min_prob)[:, None], 0.0, 1.0)
    soft_count = jnp.sum(ramp, axis=1)
    retained_sum = jnp.sum(ramp * exponent_values, axis=1)
    return top_score + jnp.log(total), retained_sum / total, jnp.log(1.0 + soft_count)


def reference(hidden_states, unembed, temp_code, minp_code):
    blocks = (hidden_states.reshape(N_DP, ROWS_DEV, D), temp_code.reshape(N_DP, ROWS_DEV), minp_code.reshape(N_DP, ROWS_DEV))
    log_norm, kept_mass, kept_count = lax.map(partial(block_stats, unembed), blocks)
    return log_norm.reshape(BATCH), kept_mass.reshape(BATCH), kept_count.reshape(BATCH)
```

```python
import functools

import jax
import jax.numpy as jnp
from jax import lax
from jax.experimental import pallas as pl
from jax.experimental.pallas import tpu as pltpu
from jax.sharding import PartitionSpec as P

MESH = pl.DeviceIdType.MESH
LANES = 128
PIECE = 16
WIDE = 256


def flip(index, bit):
    return index + bit * (1 - 2 * ((index // bit) % 2))


def kernel(
    n_dp, n_vocab,
    h_ref, w_ref, temp_ref, minp_ref,
    norm_ref, mass_ref, count_ref,
    own, weights, gathered, logits, codes_t, codes_p, inv_col, base_col, sums,
    top_col, tops, max_box, part, sum_box,
    own_sem, w_sem, ici_send, ici_recv, core_send, core_recv,
    code_send, code_recv, max_send, max_recv, sum_send, sum_recv,
):
    d = lax.axis_index("dp")
    v = lax.axis_index("vocab")
    n_all = n_dp * n_vocab
    me = d * n_vocab + v
    core = v % 2
    rows, depth = h_ref.shape
    vocab = w_ref.shape[1]
    n_roles = n_dp - 1
    n_chunks = rows // (2 * PIECE)
    chunk_rows = 2 * PIECE
    relayed = n_dp == 4

    if relayed:
        parity = (v // 2) % 2
        first = (1 - parity) * flip(d, 1) + parity * flip(d, 2)
        second = (1 - parity) * flip(d, 2) + parity * flip(d, 1)
        blocks = [first, flip(flip(d, 1), 2), second]
        targets = [(first, v), (second, v), (d, flip(v, 2))]
    else:
        blocks = [(d + n_dp - 1 - r) % n_dp for r in range(n_roles)]
        targets = [((d + 1 + r) % n_dp, v) for r in range(n_roles)]
    partner = (d, flip(v, 1))

    n_w = w_sem.shape[0]
    w_step = depth // n_w
    own_copy = pltpu.make_async_copy(h_ref, own, own_sem)
    own_copy.start()
    w_copies = []
    for i in range(n_w):
        part_of = pl.ds(i * w_step, w_step)
        w_copies.append(pltpu.make_async_copy(w_ref.at[part_of], weights.at[part_of], w_sem.at[i]))
        w_copies[-1].start()

    barrier = pltpu.get_barrier_semaphore()

    @pl.loop(1, n_all)
    def _(j):
        t = (me + j) % n_all
        pl.semaphore_signal(barrier, inc=1, device_id=(t // n_vocab, t % n_vocab), device_id_type=MESH)

    pl.semaphore_wait(barrier, n_all - 1)

    code_copies = []
    for r in range(n_roles):
        to = ((d + 1 + r) % n_dp, v)
        for s, (src, dst) in enumerate(((temp_ref, codes_t), (minp_ref, codes_p))):
            code_copies.append(pltpu.make_async_remote_copy(
                src_ref=src, dst_ref=dst.at[r], send_sem=code_send.at[s, r],
                recv_sem=code_recv.at[s, r], device_id=to, device_id_type=MESH))

    own_copy.wait()

    def own_piece(i):
        return own.at[pl.ds(pl.multiple_of(i * chunk_rows + core * PIECE, PIECE), PIECE)]

    def slot(i, r):
        return gathered.at[i, r, core]

    def send(src, i, r, sem):
        return pltpu.make_async_remote_copy(
            src_ref=src, dst_ref=slot(i, r), send_sem=sem, recv_sem=ici_recv.at[r, i],
            device_id=targets[r], device_id_type=MESH)

    def to_partner(i, r):
        return pltpu.make_async_remote_copy(
            src_ref=slot(i, r), dst_ref=slot(i, r), send_sem=core_send.at[r, i],
            recv_sem=core_recv.at[r, i], device_id=partner, device_id_type=MESH)

    direct = [0] if relayed else list(range(n_roles))
    sends = {}
    for i in range(n_chunks):
        for r in range(n_roles):
            src = own_piece(i) if r in direct else slot(i, 0)
            sends[r, i] = send(src, i, r, ici_send.at[r, i])
    passes = {(r, i): to_partner(i, r) for r in range(n_roles) for i in range(n_chunks)}
    for i in range(n_chunks):
        for r in direct:
            sends[r, i].start()
    for c in code_copies:
        c.start()

    def local_max(values):
        return functools.reduce(jnp.maximum, [values[:, t * LANES:(t + 1) * LANES] for t in range(WIDE // LANES)])

    def to_row(values, op):
        return op(values.T, axis=0, keepdims=True)

    for c in w_copies:
        c.wait()

    def own_step(n, best):
        cols = pl.ds(pl.multiple_of(n * WIDE, WIDE), WIDE)
        out = jnp.dot(own[...], weights[:, cols], preferred_element_type=jnp.float32)
        logits[0, :, cols] = out
        return jnp.maximum(best, local_max(out))

    best = lax.fori_loop(0, vocab // WIDE, own_step, jnp.full((rows, LANES), -jnp.inf, jnp.float32))
    max_box[0, pl.ds(d, 1), :] = to_row(best, jnp.max)

    def column(row):
        return jnp.broadcast_to(row, (LANES, LANES)).T

    def keep_columns(r, temp, minp):
        inv_col[r] = column(1.0 / (temp.astype(jnp.float32) * 0.01))
        base_col[r] = column(1.0 - jnp.log(minp.astype(jnp.float32) * 0.01))

    keep_columns(0, temp_ref[...], minp_ref[...])

    group = max(n_chunks // 2, 1)
    for g in range(n_chunks // group):
        chunks = range(g * group, (g + 1) * group)
        for i in chunks:
            for r in direct:
                sends[r, i].wait_recv()
                if relayed:
                    sends[1, i].start()
                    sends[2, i].start()
                passes[r, i].start()
        for i in chunks:
            for r in range(n_roles):
                if r not in direct:
                    sends[r, i].wait_recv()
                    passes[r, i].start()
        if g == 0:
            for c in code_copies:
                c.wait()
            for r in range(n_roles):
                s = ((d + n_dp - blocks[r]) % n_dp) - 1
                keep_columns(r + 1, codes_t[s], codes_p[s])
        for i in chunks:
            for r in range(n_roles):
                passes[r, i].wait_recv()
        many = group * n_roles * chunk_rows

        def step(n, best):
            cols = pl.ds(pl.multiple_of(n * WIDE, WIDE), WIDE)
            lhs = gathered[g * group:(g + 1) * group].reshape(many, depth)
            out = jnp.dot(lhs, weights[:, cols], preferred_element_type=jnp.float32)
            for a, i in enumerate(chunks):
                for r in range(n_roles):
                    at = (a * n_roles + r) * chunk_rows
                    logits[r + 1, i * chunk_rows:(i + 1) * chunk_rows, cols] = out[at:at + chunk_rows]
            return jnp.maximum(best, local_max(out))

        best = lax.fori_loop(0, vocab // WIDE, step, jnp.full((many, LANES), -jnp.inf, jnp.float32))
        for r in range(n_roles):
            rows_r = [best[(a * n_roles + r) * chunk_rows:(a * n_roles + r + 1) * chunk_rows] for a in range(group)]
            piece = jnp.concatenate(rows_r, axis=0)
            wide = group * chunk_rows
            max_box[0, pl.ds(blocks[r], 1), g * wide:(g + 1) * wide] = to_row(piece, jnp.max)

    def exchange(source, box, send_sem, recv_sem):
        def copy(j):
            t = (me + j) % n_all
            return pltpu.make_async_remote_copy(
                src_ref=source(t // n_vocab), dst_ref=box.at[j], send_sem=send_sem, recv_sem=recv_sem,
                device_id=(t // n_vocab, t % n_vocab), device_id_type=MESH)

        @pl.loop(1, n_all)
        def _(j):
            copy(j).start()

        rest = box.at[pl.ds(1, n_all - 1)]
        return pltpu.make_async_copy(rest, rest, send_sem), pltpu.make_async_copy(rest, rest, recv_sem)

    max_sent, max_got = exchange(lambda block: max_box.at[0], max_box, max_send, max_recv)
    max_got.wait()
    tops[...] = jnp.max(max_box[...], axis=0)
    max_sent.wait()

    lane_tiles = vocab // LANES
    strip = 32
    for r in range(n_dp):
        block = d if r == 0 else blocks[r - 1]
        top_col[...] = column(tops[pl.ds(block, 1), :])

        @pl.loop(0, rows // strip)
        def _(q):
            at = pl.ds(pl.multiple_of(q * strip, strip), strip)
            top, inv, base = top_col[at], inv_col[r, at], base_col[r, at]
            total = count = mass = jnp.zeros((strip, LANES), jnp.float32)
            for t in range(lane_tiles):
                below = (logits[r, at, t * LANES:(t + 1) * LANES] - top) * inv
                term = jnp.exp(below)
                ramp = jnp.clip(below + base, 0.0, 1.0)
                total, count, mass = total + term, count + ramp, mass + ramp * term
            sums[0, at], sums[1, at], sums[2, at] = total, count, mass

        rows_of = [to_row(sums[s], jnp.sum) for s in range(3)]
        part[pl.ds(block, 1)] = jnp.concatenate(rows_of + [jnp.zeros_like(rows_of[0])], axis=0)[None]

    sum_box[0] = part[d]
    sum_sent, sum_got = exchange(lambda block: part.at[block], sum_box, sum_send, sum_recv)
    temperature = temp_ref[...].astype(jnp.float32) * 0.01
    top_score = tops[pl.ds(d, 1), :] / temperature
    sum_got.wait()
    whole = jnp.sum(sum_box[...], axis=0)
    total, count, mass = whole[0:1], whole[1:2], whole[2:3]
    norm_ref[...] = top_score + jnp.log(total)
    mass_ref[...] = mass / total
    count_ref[...] = jnp.log(1.0 + count)

    sum_sent.wait()
    for c in (*sends.values(), *passes.values()):
        c.wait_send()


def on_device(n_dp, n_vocab, hidden_states, unembed, temp_code, minp_code):
    rows, depth = hidden_states.shape
    vocab = unembed.shape[1]
    n_all = n_dp * n_vocab
    n_roles = n_dp - 1
    n_chunks = rows // (2 * PIECE)
    f32, i32, bf16 = jnp.float32, jnp.int32, hidden_states.dtype
    dma = pltpu.SemaphoreType.DMA
    vmem = pl.BlockSpec(memory_space=pltpu.VMEM)
    any_space = pl.BlockSpec(memory_space=pl.ANY)
    outs = pl.pallas_call(
        functools.partial(kernel, n_dp, n_vocab),
        out_shape=[jax.ShapeDtypeStruct((1, rows), f32)] * 3,
        in_specs=[any_space, any_space, vmem, vmem],
        out_specs=[vmem] * 3,
        scratch_shapes=[
            pltpu.VMEM((rows, depth), bf16),
            pltpu.VMEM((depth, vocab), bf16),
            pltpu.VMEM((n_chunks, n_roles, 2, PIECE, depth), bf16),
            pltpu.VMEM((n_dp, rows, vocab), f32),
            pltpu.VMEM((n_roles, 1, rows), i32),
            pltpu.VMEM((n_roles, 1, rows), i32),
            pltpu.VMEM((n_dp, rows, LANES), f32),
            pltpu.VMEM((n_dp, rows, LANES), f32),
            pltpu.VMEM((3, rows, LANES), f32),
            pltpu.VMEM((rows, LANES), f32),
            pltpu.VMEM((n_dp, rows), f32),
            pltpu.VMEM((n_all, n_dp, rows), f32),
            pltpu.VMEM((n_dp, 4, rows), f32),
            pltpu.VMEM((n_all, 4, rows), f32),
            dma, dma((4,)),
            dma((n_roles, n_chunks)), dma((n_roles, n_chunks)),
            dma((n_roles, n_chunks)), dma((n_roles, n_chunks)),
            dma((2, n_roles)), dma((2, n_roles)),
            dma, dma, dma, dma,
        ],
        compiler_params=pltpu.CompilerParams(collective_id=0, has_side_effects=True),
    )(hidden_states, unembed, temp_code.reshape(1, rows), minp_code.reshape(1, rows))
    return tuple(o.reshape(rows) for o in outs)


def solution(mesh):
    in_specs = (P("dp", None), P(None, ("dp", "vocab")), P("dp"), P("dp"))
    out_specs = (P("dp"), P("dp"), P("dp"))
    body = functools.partial(on_device, mesh.shape["dp"], mesh.shape["vocab"])
    return jax.shard_map(body, mesh=mesh, in_specs=in_specs, out_specs=out_specs, check_vma=False)
```

```python
import functools

import jax
import jax.numpy as jnp
from jax import lax
from jax.experimental import pallas as pl
from jax.experimental.pallas import tpu as pltpu
from jax.sharding import PartitionSpec as P

MESH = pl.DeviceIdType.MESH
LANES = 128
PIECE = 16
SPLIT = 2
WIDE = 256


def flip(index, bit):
    return index + bit * (1 - 2 * ((index // bit) % 2))


def kernel(
    n_dp, n_vocab,
    h_ref, w_ref, temp_ref, minp_ref,
    out_ref,
    own, weights, gathered, logits, codes_t, codes_p, inv_col, base_col, sums,
    top_col, tops, max_box, part, sum_box,
    own_sem, w_sem, ici_send, ici_recv, core_send, core_recv,
    code_send, code_recv, max_send, max_recv, sum_send, sum_recv, seen,
):
    d = lax.axis_index("dp")
    v = lax.axis_index("vocab")
    n_all = n_dp * n_vocab
    me = d * n_vocab + v
    core = v % 2
    rows, depth = h_ref.shape
    vocab = w_ref.shape[1]
    n_roles = n_dp - 1
    n_chunks = rows // (2 * PIECE)
    chunk_rows = 2 * PIECE
    relayed = n_dp == 4

    if relayed:
        parity = (v // 2) % 2
        first = (1 - parity) * flip(d, 1) + parity * flip(d, 2)
        second = (1 - parity) * flip(d, 2) + parity * flip(d, 1)
        blocks = [first, flip(flip(d, 1), 2), second]
        targets = [(first, v), (second, v), (d, flip(v, 2))]
        near = [[(flip(d, 1), v)], [(flip(d, 2), v)]]
    else:
        blocks = [(d + n_dp - 1 - r) % n_dp for r in range(n_roles)]
        targets = [((d + 1 + r) % n_dp, v) for r in range(n_roles)]
        near = [targets]
    partner = (d, flip(v, 1))

    n_w = w_sem.shape[0]
    w_step = depth // n_w
    own_copy = pltpu.make_async_copy(h_ref, own, own_sem)
    own_copy.start()
    w_copies = []
    for i in range(n_w):
        part_of = pl.ds(i * w_step, w_step)
        w_copies.append(pltpu.make_async_copy(w_ref.at[part_of], weights.at[part_of], w_sem.at[i]))

    barrier = pltpu.get_barrier_semaphore()
    line = v // 2
    has_low = line > 0
    has_high = line < n_vocab // 2 - 1
    ends = has_low.astype(jnp.int32) + has_high.astype(jnp.int32)

    def signal(sem, to):
        pl.semaphore_signal(sem, inc=1, device_id=to, device_id_type=MESH)

    def signal_line(sem):
        @pl.when(has_low)
        def _():
            signal(sem, (d, v - 2))

        @pl.when(has_high)
        def _():
            signal(sem, (d, v + 2))

    direct_peers = [to for stage in near for to in stage] + [partner]
    for to in direct_peers:
        signal(barrier, to)
    signal_line(barrier)
    for c in w_copies:
        c.start()
    pl.semaphore_wait(barrier, len(direct_peers) + ends)

    def line_round(k):
        def run():
            signal_line(seen.at[k])
            pl.semaphore_wait(seen.at[k], ends)
        return run

    def peer_round(k, peers):
        def run():
            for to in peers:
                signal(seen.at[k], to)
            pl.semaphore_wait(seen.at[k], len(peers))
        return run

    n_line = n_vocab // 2 - 2
    chores = [line_round(k) for k in range(n_line)]
    for k, peers in enumerate(near + [[partner]]):
        chores.append(peer_round(n_line + k, peers))

    code_copies = []
    for r in range(n_roles):
        to = ((d + 1 + r) % n_dp, v)
        for s, (src, dst) in enumerate(((temp_ref, codes_t), (minp_ref, codes_p))):
            code_copies.append(pltpu.make_async_remote_copy(
                src_ref=src, dst_ref=dst.at[r], send_sem=code_send.at[s, r],
                recv_sem=code_recv.at[s, r], device_id=to, device_id_type=MESH))

    def start_codes():
        for c in code_copies:
            c.start()

    chores.append(start_codes)

    def chore(count=1):
        for _ in range(min(count, len(chores))):
            chores.pop(0)()

    n_units = n_chunks * SPLIT
    width = depth // SPLIT

    def own_piece(u):
        at = pl.multiple_of((u // SPLIT) * chunk_rows + core * PIECE, PIECE)
        return own.at[pl.ds(at, PIECE), pl.ds((u % SPLIT) * width, width)]

    def slot(u, r):
        return gathered.at[u // SPLIT, r, core, :, pl.ds((u % SPLIT) * width, width)]

    def send(src, u, r, sem):
        return pltpu.make_async_remote_copy(
            src_ref=src, dst_ref=slot(u, r), send_sem=sem, recv_sem=ici_recv.at[r, u],
            device_id=targets[r], device_id_type=MESH)

    def to_partner(u, r):
        return pltpu.make_async_remote_copy(
            src_ref=slot(u, r), dst_ref=slot(u, r), send_sem=core_send.at[r, u],
            recv_sem=core_recv.at[r, u], device_id=partner, device_id_type=MESH)

    direct = [0] if relayed else list(range(n_roles))
    others = [r for r in range(n_roles) if r not in direct]
    sends = {}
    for u in range(n_units):
        for r in range(n_roles):
            src = own_piece(u) if r in direct else slot(u, 0)
            sends[r, u] = send(src, u, r, ici_send.at[r, u])
    passes = {(r, u): to_partner(u, r) for r in range(n_roles) for u in range(n_units)}
    own_copy.wait()
    for u in range(n_units):
        for r in direct:
            sends[r, u].start()
    chore()

    def take_direct(u):
        for r in direct:
            sends[r, u].wait_recv()
            for o in others:
                sends[o, u].start()
            passes[r, u].start()

    def take_others(u):
        for r in others:
            sends[r, u].wait_recv()
            passes[r, u].start()

    def local_max(values):
        return functools.reduce(jnp.maximum, [values[:, t * LANES:(t + 1) * LANES] for t in range(WIDE // LANES)])

    def to_row(values, op):
        return op(values.T, axis=0, keepdims=True)

    take_direct(0)
    for c in w_copies:
        c.wait()

    def own_step(n, best):
        cols = pl.ds(pl.multiple_of(n * WIDE, WIDE), WIDE)
        out = jnp.dot(own[...], weights[:, cols], preferred_element_type=jnp.float32)
        logits[0, :, cols] = out
        return jnp.maximum(best, local_max(out))

    best = lax.fori_loop(0, vocab // WIDE, own_step, jnp.full((rows, LANES), -jnp.inf, jnp.float32))
    max_box[0, pl.ds(d, 1), :] = to_row(best, jnp.max)

    def column(row):
        return jnp.broadcast_to(row, (LANES, LANES)).T

    def keep_columns(r, temp, minp):
        inv_col[r] = column(1.0 / (temp.astype(jnp.float32) * 0.01))
        base_col[r] = column(1.0 - jnp.log(minp.astype(jnp.float32) * 0.01))

    keep_columns(0, temp_ref[...], minp_ref[...])

    for u in range(1, n_units):
        take_direct(u)
        chore()
        take_others(u - 1)
    chore(len(chores))

    for chunks in (range(n_chunks - 1), range(n_chunks - 1, n_chunks)):
        g, group = chunks[0], len(chunks)
        if g:
            take_others(n_units - 1)
        else:
            for c in code_copies:
                c.wait()
            for r in range(n_roles):
                s = ((d + n_dp - blocks[r]) % n_dp) - 1
                keep_columns(r + 1, codes_t[s], codes_p[s])
        for u in range(g * SPLIT, (g + group) * SPLIT):
            for r in range(n_roles):
                passes[r, u].wait_recv()
        many = group * n_roles * chunk_rows

        def step(n, best):
            cols = pl.ds(pl.multiple_of(n * WIDE, WIDE), WIDE)
            lhs = gathered[g:g + group].reshape(many, depth)
            out = jnp.dot(lhs, weights[:, cols], preferred_element_type=jnp.float32)
            for a, i in enumerate(chunks):
                for r in range(n_roles):
                    at = (a * n_roles + r) * chunk_rows
                    logits[r + 1, i * chunk_rows:(i + 1) * chunk_rows, cols] = out[at:at + chunk_rows]
            return jnp.maximum(best, local_max(out))

        best = lax.fori_loop(0, vocab // WIDE, step, jnp.full((many, LANES), -jnp.inf, jnp.float32))
        for r in range(n_roles):
            rows_r = [best[(a * n_roles + r) * chunk_rows:(a * n_roles + r + 1) * chunk_rows] for a in range(group)]
            piece = jnp.concatenate(rows_r, axis=0)
            max_box[0, pl.ds(blocks[r], 1), g * chunk_rows:(g + group) * chunk_rows] = to_row(piece, jnp.max)

    def exchange(source, box, send_sem, recv_sem):
        def send_row(down, skip):
            to_d = (d + down) % n_dp
            for across in reversed(range(skip, n_vocab)):
                pltpu.make_async_remote_copy(
                    src_ref=source(to_d), dst_ref=box.at[down * n_vocab + across],
                    send_sem=send_sem, recv_sem=recv_sem,
                    device_id=(to_d, (v + across) % n_vocab), device_id_type=MESH).start()

        if n_dp > 4:
            pl.loop(1, n_dp)(lambda down: send_row(down, 0))
        else:
            for down in range(1, n_dp):
                send_row(down, 0)
        send_row(0, 1)

        rest = box.at[pl.ds(1, n_all - 1)]
        return pltpu.make_async_copy(rest, rest, send_sem), pltpu.make_async_copy(rest, rest, recv_sem)

    max_sent, max_got = exchange(lambda block: max_box.at[0], max_box, max_send, max_recv)
    max_got.wait()
    tops[...] = jnp.max(max_box[...], axis=0)
    max_sent.wait()

    lane_tiles = vocab // LANES
    strip = 32
    for r in range(n_dp):
        block = d if r == 0 else blocks[r - 1]
        top_col[...] = column(tops[pl.ds(block, 1), :])

        @pl.loop(0, rows // strip)
        def _(q):
            at = pl.ds(pl.multiple_of(q * strip, strip), strip)
            top, inv, base = top_col[at], inv_col[r, at], base_col[r, at]
            total = count = mass = jnp.zeros((strip, LANES), jnp.float32)
            for t in range(lane_tiles):
                below = (logits[r, at, t * LANES:(t + 1) * LANES] - top) * inv
                term = jnp.exp(below)
                ramp = jnp.clip(below + base, 0.0, 1.0)
                total, count, mass = total + term, count + ramp, mass + ramp * term
            sums[0, at], sums[1, at], sums[2, at] = total, count, mass

        rows_of = [to_row(sums[s], jnp.sum) for s in range(3)]
        part[pl.ds(block, 1)] = jnp.concatenate(rows_of + [jnp.zeros_like(rows_of[0])], axis=0)[None]

    sum_box[0] = part[d]
    sum_sent, sum_got = exchange(lambda block: part.at[block], sum_box, sum_send, sum_recv)
    temperature = temp_ref[...].astype(jnp.float32) * 0.01
    top_score = tops[pl.ds(d, 1), :] / temperature
    sum_got.wait()
    whole = jnp.sum(sum_box[...], axis=0)
    total, count, mass = whole[0:1], whole[1:2], whole[2:3]
    out_ref[0:1] = top_score + jnp.log(total)
    out_ref[1:2] = mass / total
    out_ref[2:3] = jnp.log(1.0 + count)

    sum_sent.wait()
    for c in (*sends.values(), *passes.values()):
        c.wait_send()


def on_device(n_dp, n_vocab, hidden_states, unembed, temp_code, minp_code):
    rows, depth = hidden_states.shape
    vocab = unembed.shape[1]
    n_all = n_dp * n_vocab
    n_roles = n_dp - 1
    n_chunks = rows // (2 * PIECE)
    f32, i32, bf16 = jnp.float32, jnp.int32, hidden_states.dtype
    dma = pltpu.SemaphoreType.DMA
    vmem = pl.BlockSpec(memory_space=pltpu.VMEM)
    any_space = pl.BlockSpec(memory_space=pl.ANY)
    outs = pl.pallas_call(
        functools.partial(kernel, n_dp, n_vocab),
        out_shape=jax.ShapeDtypeStruct((3, rows), f32),
        in_specs=[any_space, any_space, vmem, vmem],
        out_specs=vmem,
        scratch_shapes=[
            pltpu.VMEM((rows, depth), bf16),
            pltpu.VMEM((depth, vocab), bf16),
            pltpu.VMEM((n_chunks, n_roles, 2, PIECE, depth), bf16),
            pltpu.VMEM((n_dp, rows, vocab), f32),
            pltpu.VMEM((n_roles, 1, rows), i32),
            pltpu.VMEM((n_roles, 1, rows), i32),
            pltpu.VMEM((n_dp, rows, LANES), f32),
            pltpu.VMEM((n_dp, rows, LANES), f32),
            pltpu.VMEM((3, rows, LANES), f32),
            pltpu.VMEM((rows, LANES), f32),
            pltpu.VMEM((n_dp, rows), f32),
            pltpu.VMEM((n_all, n_dp, rows), f32),
            pltpu.VMEM((n_dp, 4, rows), f32),
            pltpu.VMEM((n_all, 4, rows), f32),
            dma, dma((4,)),
            *[dma((n_roles, n_chunks * SPLIT))] * 4,
            dma((2, n_roles)), dma((2, n_roles)),
            dma, dma, dma, dma,
            pltpu.SemaphoreType.REGULAR((n_vocab // 2 + 1,)),
        ],
        compiler_params=pltpu.CompilerParams(collective_id=0, has_side_effects=True),
    )(hidden_states, unembed, temp_code.reshape(1, rows), minp_code.reshape(1, rows))
    return outs[0], outs[1], outs[2]


def solution(mesh):
    in_specs = (P("dp", None), P(None, ("dp", "vocab")), P("dp"), P("dp"))
    out_specs = (P("dp"), P("dp"), P("dp"))
    body = functools.partial(on_device, mesh.shape["dp"], mesh.shape["vocab"])
    return jax.shard_map(body, mesh=mesh, in_specs=in_specs, out_specs=out_specs, check_vma=False)
```

```python
import functools

import jax
import jax.numpy as jnp
from jax import lax
from jax.experimental import pallas as pl
from jax.experimental.pallas import tpu as pltpu
from jax.sharding import PartitionSpec as P

MESH = pl.DeviceIdType.MESH
LANES = 128
PIECE = 16
SPLIT = 1
WIDE = 256


def flip(index, bit):
    return index + bit * (1 - 2 * ((index // bit) % 2))


def kernel(
    n_dp, n_vocab,
    h_ref, w_ref, temp_ref, minp_ref,
    out_ref,
    own, weights, gathered, logits, codes_t, codes_p, inv_col, base_col, sums,
    top_col, tops, max_box, part, sum_box,
    own_sem, w_sem, ici_send, ici_recv, core_send, core_recv,
    code_send, code_recv, max_send, max_recv, sum_send, sum_recv, seen,
):
    d = lax.axis_index("dp")
    v = lax.axis_index("vocab")
    n_all = n_dp * n_vocab
    me = d * n_vocab + v
    core = v % 2
    rows, depth = h_ref.shape
    vocab = w_ref.shape[1]
    n_roles = n_dp - 1
    n_chunks = rows // (2 * PIECE)
    chunk_rows = 2 * PIECE
    relayed = n_dp == 4

    if relayed:
        parity = (v // 2) % 2
        first = (1 - parity) * flip(d, 1) + parity * flip(d, 2)
        second = (1 - parity) * flip(d, 2) + parity * flip(d, 1)
        blocks = [first, flip(flip(d, 1), 2), second]
        targets = [(first, v), (second, v), (d, flip(v, 2))]
        near = [[(flip(d, 1), v)], [(flip(d, 2), v)]]
    else:
        blocks = [(d + n_dp - 1 - r) % n_dp for r in range(n_roles)]
        targets = [((d + 1 + r) % n_dp, v) for r in range(n_roles)]
        near = [targets]
    partner = (d, flip(v, 1))

    n_w = w_sem.shape[0]
    w_step = depth // n_w
    own_copy = pltpu.make_async_copy(h_ref, own, own_sem)
    own_copy.start()
    w_copies = []
    for i in range(n_w):
        part_of = pl.ds(i * w_step, w_step)
        w_copies.append(pltpu.make_async_copy(w_ref.at[part_of], weights.at[part_of], w_sem.at[i]))

    barrier = pltpu.get_barrier_semaphore()
    line = v // 2
    has_low = line > 0
    has_high = line < n_vocab // 2 - 1
    ends = has_low.astype(jnp.int32) + has_high.astype(jnp.int32)

    def signal(sem, to):
        pl.semaphore_signal(sem, inc=1, device_id=to, device_id_type=MESH)

    def signal_line(sem):
        @pl.when(has_low)
        def _():
            signal(sem, (d, v - 2))

        @pl.when(has_high)
        def _():
            signal(sem, (d, v + 2))

    direct_peers = [to for stage in near for to in stage] + [partner]
    for to in direct_peers:
        signal(barrier, to)
    signal_line(barrier)
    for c in w_copies:
        c.start()
    pl.semaphore_wait(barrier, len(direct_peers) + ends)

    def line_round(k):
        def run():
            signal_line(seen.at[k])
            pl.semaphore_wait(seen.at[k], ends)
        return run

    def peer_round(k, peers):
        def run():
            for to in peers:
                signal(seen.at[k], to)
            pl.semaphore_wait(seen.at[k], len(peers))
        return run

    n_line = n_vocab // 2 - 2
    chores = [line_round(k) for k in range(n_line)]
    for k, peers in enumerate(near + [[partner]]):
        chores.append(peer_round(n_line + k, peers))

    code_copies = []
    for r in range(n_roles):
        to = ((d + 1 + r) % n_dp, v)
        for s, (src, dst) in enumerate(((temp_ref, codes_t), (minp_ref, codes_p))):
            code_copies.append(pltpu.make_async_remote_copy(
                src_ref=src, dst_ref=dst.at[r], send_sem=code_send.at[s, r],
                recv_sem=code_recv.at[s, r], device_id=to, device_id_type=MESH))

    def start_codes():
        for c in code_copies:
            c.start()

    chores.append(start_codes)

    def chore(count=1):
        for _ in range(min(count, len(chores))):
            chores.pop(0)()

    n_units = n_chunks * SPLIT
    width = depth // SPLIT

    def own_piece(u):
        at = pl.multiple_of((u // SPLIT) * chunk_rows + core * PIECE, PIECE)
        return own.at[pl.ds(at, PIECE), pl.ds((u % SPLIT) * width, width)]

    def slot(u, r):
        return gathered.at[u // SPLIT, r, core, :, pl.ds((u % SPLIT) * width, width)]

    def send(src, u, r, sem):
        return pltpu.make_async_remote_copy(
            src_ref=src, dst_ref=slot(u, r), send_sem=sem, recv_sem=ici_recv.at[r, u],
            device_id=targets[r], device_id_type=MESH)

    def to_partner(u, r):
        return pltpu.make_async_remote_copy(
            src_ref=slot(u, r), dst_ref=slot(u, r), send_sem=core_send.at[r, u],
            recv_sem=core_recv.at[r, u], device_id=partner, device_id_type=MESH)

    direct = [0] if relayed else list(range(n_roles))
    others = [r for r in range(n_roles) if r not in direct]
    sends = {}
    for u in range(n_units):
        for r in range(n_roles):
            src = own_piece(u) if r in direct else slot(u, 0)
            sends[r, u] = send(src, u, r, ici_send.at[r, u])
    passes = {(r, u): to_partner(u, r) for r in range(n_roles) for u in range(n_units)}
    own_copy.wait()
    for u in range(n_units):
        for r in direct:
            sends[r, u].start()
    chore()

    def take_direct(u):
        for r in direct:
            sends[r, u].wait_recv()
            for o in others:
                sends[o, u].start()
            passes[r, u].start()

    def take_others(u):
        for r in others:
            sends[r, u].wait_recv()
            passes[r, u].start()

    def local_max(values):
        return functools.reduce(jnp.maximum, [values[:, t * LANES:(t + 1) * LANES] for t in range(WIDE // LANES)])

    def to_row(values, op):
        return op(values.T, axis=0, keepdims=True)

    take_direct(0)
    for c in w_copies:
        c.wait()

    def own_step(n, best):
        cols = pl.ds(pl.multiple_of(n * WIDE, WIDE), WIDE)
        out = jnp.dot(own[...], weights[:, cols], preferred_element_type=jnp.float32)
        logits[0, :, cols] = out
        return jnp.maximum(best, local_max(out))

    best = lax.fori_loop(0, vocab // WIDE, own_step, jnp.full((rows, LANES), -jnp.inf, jnp.float32))
    max_box[0, pl.ds(d, 1), :] = to_row(best, jnp.max)

    def column(row):
        return jnp.broadcast_to(row, (LANES, LANES)).T

    def keep_columns(r, temp, minp):
        inv_col[r] = column(1.0 / (temp.astype(jnp.float32) * 0.01))
        base_col[r] = column(1.0 - jnp.log(minp.astype(jnp.float32) * 0.01))

    keep_columns(0, temp_ref[...], minp_ref[...])

    early = max(n_chunks - 2, 1)
    for u in range(1, n_units):
        take_direct(u)
        chore()
        if u <= early * SPLIT:
            take_others(u - 1)
    chore(len(chores))

    for chunks in [range(early)] + [range(i, i + 1) for i in range(early, n_chunks)]:
        g, group = chunks[0], len(chunks)
        if g:
            for u in range(g * SPLIT, (g + 1) * SPLIT):
                take_others(u)
        if g == early:
            for c in code_copies:
                c.wait()
            for r in range(n_roles):
                s = ((d + n_dp - blocks[r]) % n_dp) - 1
                keep_columns(r + 1, codes_t[s], codes_p[s])
        for u in range(g * SPLIT, (g + group) * SPLIT):
            for r in range(n_roles):
                passes[r, u].wait_recv()
        many = group * n_roles * chunk_rows

        def step(n, best):
            cols = pl.ds(pl.multiple_of(n * WIDE, WIDE), WIDE)
            lhs = gathered[g:g + group].reshape(many, depth)
            out = jnp.dot(lhs, weights[:, cols], preferred_element_type=jnp.float32)
            for a, i in enumerate(chunks):
                for r in range(n_roles):
                    at = (a * n_roles + r) * chunk_rows
                    logits[r + 1, i * chunk_rows:(i + 1) * chunk_rows, cols] = out[at:at + chunk_rows]
            return jnp.maximum(best, local_max(out))

        best = lax.fori_loop(0, vocab // WIDE, step, jnp.full((many, LANES), -jnp.inf, jnp.float32))
        for r in range(n_roles):
            rows_r = [best[(a * n_roles + r) * chunk_rows:(a * n_roles + r + 1) * chunk_rows] for a in range(group)]
            piece = jnp.concatenate(rows_r, axis=0)
            max_box[0, pl.ds(blocks[r], 1), g * chunk_rows:(g + group) * chunk_rows] = to_row(piece, jnp.max)

    def exchange(source, box, send_sem, recv_sem):
        def send_row(down, skip):
            to_d = (d + down) % n_dp
            for across in reversed(range(skip, n_vocab)):
                pltpu.make_async_remote_copy(
                    src_ref=source(to_d), dst_ref=box.at[down * n_vocab + across],
                    send_sem=send_sem, recv_sem=recv_sem,
                    device_id=(to_d, (v + across) % n_vocab), device_id_type=MESH).start()

        if n_dp > 4:
            pl.loop(1, n_dp)(lambda down: send_row(down, 0))
        else:
            for down in range(1, n_dp):
                send_row(down, 0)
        send_row(0, 1)

        rest = box.at[pl.ds(1, n_all - 1)]
        return pltpu.make_async_copy(rest, rest, send_sem), pltpu.make_async_copy(rest, rest, recv_sem)

    max_sent, max_got = exchange(lambda block: max_box.at[0], max_box, max_send, max_recv)
    max_got.wait()
    tops[...] = jnp.max(max_box[...], axis=0)
    max_sent.wait()

    lane_tiles = vocab // LANES
    strip = 32
    for r in range(n_dp):
        block = d if r == 0 else blocks[r - 1]
        top_col[...] = column(tops[pl.ds(block, 1), :])

        @pl.loop(0, rows // strip)
        def _(q):
            at = pl.ds(pl.multiple_of(q * strip, strip), strip)
            top, inv, base = top_col[at], inv_col[r, at], base_col[r, at]
            total = count = mass = jnp.zeros((strip, LANES), jnp.float32)
            for t in range(lane_tiles):
                below = (logits[r, at, t * LANES:(t + 1) * LANES] - top) * inv
                term = jnp.exp(below)
                ramp = jnp.clip(below + base, 0.0, 1.0)
                total, count, mass = total + term, count + ramp, mass + ramp * term
            sums[0, at], sums[1, at], sums[2, at] = total, count, mass

        rows_of = [to_row(sums[s], jnp.sum) for s in range(3)]
        part[pl.ds(block, 1)] = jnp.concatenate(rows_of + [jnp.zeros_like(rows_of[0])], axis=0)[None]

    sum_box[0] = part[d]
    sum_sent, sum_got = exchange(lambda block: part.at[block], sum_box, sum_send, sum_recv)
    temperature = temp_ref[...].astype(jnp.float32) * 0.01
    top_score = tops[pl.ds(d, 1), :] / temperature
    sum_got.wait()
    whole = jnp.sum(sum_box[...], axis=0)
    total, count, mass = whole[0:1], whole[1:2], whole[2:3]
    out_ref[0:1] = top_score + jnp.log(total)
    out_ref[1:2] = mass / total
    out_ref[2:3] = jnp.log(1.0 + count)

    sum_sent.wait()
    for c in (*sends.values(), *passes.values()):
        c.wait_send()


def on_device(n_dp, n_vocab, hidden_states, unembed, temp_code, minp_code):
    rows, depth = hidden_states.shape
    vocab = unembed.shape[1]
    n_all = n_dp * n_vocab
    n_roles = n_dp - 1
    n_chunks = rows // (2 * PIECE)
    f32, i32, bf16 = jnp.float32, jnp.int32, hidden_states.dtype
    dma = pltpu.SemaphoreType.DMA
    vmem = pl.BlockSpec(memory_space=pltpu.VMEM)
    any_space = pl.BlockSpec(memory_space=pl.ANY)
    outs = pl.pallas_call(
        functools.partial(kernel, n_dp, n_vocab),
        out_shape=jax.ShapeDtypeStruct((3, rows), f32),
        in_specs=[any_space, any_space, vmem, vmem],
        out_specs=vmem,
        scratch_shapes=[
            pltpu.VMEM((rows, depth), bf16),
            pltpu.VMEM((depth, vocab), bf16),
            pltpu.VMEM((n_chunks, n_roles, 2, PIECE, depth), bf16),
            pltpu.VMEM((n_dp, rows, vocab), f32),
            pltpu.VMEM((n_roles, 1, rows), i32),
            pltpu.VMEM((n_roles, 1, rows), i32),
            pltpu.VMEM((n_dp, rows, LANES), f32),
            pltpu.VMEM((n_dp, rows, LANES), f32),
            pltpu.VMEM((3, rows, LANES), f32),
            pltpu.VMEM((rows, LANES), f32),
            pltpu.VMEM((n_dp, rows), f32),
            pltpu.VMEM((n_all, n_dp, rows), f32),
            pltpu.VMEM((n_dp, 4, rows), f32),
            pltpu.VMEM((n_all, 4, rows), f32),
            dma, dma((4,)),
            *[dma((n_roles, n_chunks * SPLIT))] * 4,
            dma((2, n_roles)), dma((2, n_roles)),
            dma, dma, dma, dma,
            pltpu.SemaphoreType.REGULAR((n_vocab // 2 + 1,)),
        ],
        compiler_params=pltpu.CompilerParams(collective_id=0, has_side_effects=True),
    )(hidden_states, unembed, temp_code.reshape(1, rows), minp_code.reshape(1, rows))
    return outs[0], outs[1], outs[2]


def solution(mesh):
    in_specs = (P("dp", None), P(None, ("dp", "vocab")), P("dp"), P("dp"))
    out_specs = (P("dp"), P("dp"), P("dp"))
    body = functools.partial(on_device, mesh.shape["dp"], mesh.shape["vocab"])
    return jax.shard_map(body, mesh=mesh, in_specs=in_specs, out_specs=out_specs, check_vma=False)
```

```python
import functools

import jax
import jax.numpy as jnp
from jax import lax
from jax.experimental import pallas as pl
from jax.experimental.pallas import tpu as pltpu
from jax.sharding import PartitionSpec as P

MESH = pl.DeviceIdType.MESH
LANES = 128
PIECE = 16
SPLIT = 1
WIDE = 256


def flip(index, bit):
    return index + bit * (1 - 2 * ((index // bit) % 2))


def kernel(
    n_dp, n_vocab,
    h_ref, w_ref, temp_ref, minp_ref,
    out_ref,
    own, weights, gathered, logits, codes_t, codes_p, inv_col, base_col, sums,
    top_col, tops, max_box, part, sum_box,
    own_sem, w_sem, ici_send, ici_recv, core_send, core_recv,
    code_send, code_recv, max_send, max_recv, sum_send, sum_recv, seen,
):
    d = lax.axis_index("dp")
    v = lax.axis_index("vocab")
    n_all = n_dp * n_vocab
    me = d * n_vocab + v
    core = v % 2
    rows, depth = h_ref.shape
    vocab = w_ref.shape[1]
    n_roles = n_dp - 1
    n_chunks = rows // (2 * PIECE)
    chunk_rows = 2 * PIECE
    relayed = n_dp == 4

    if relayed:
        parity = (v // 2) % 2
        first = (1 - parity) * flip(d, 1) + parity * flip(d, 2)
        second = (1 - parity) * flip(d, 2) + parity * flip(d, 1)
        blocks = [first, flip(flip(d, 1), 2), second]
        targets = [(first, v), (second, v), (d, flip(v, 2))]
        near = [[(flip(d, 1), v)], [(flip(d, 2), v)]]
    else:
        blocks = [(d + n_dp - 1 - r) % n_dp for r in range(n_roles)]
        targets = [((d + 1 + r) % n_dp, v) for r in range(n_roles)]
        near = [targets]
    partner = (d, flip(v, 1))

    n_w = w_sem.shape[0]
    w_step = depth // n_w
    own_copy = pltpu.make_async_copy(h_ref, own, own_sem)
    own_copy.start()
    w_copies = []
    for i in range(n_w):
        part_of = pl.ds(i * w_step, w_step)
        w_copies.append(pltpu.make_async_copy(w_ref.at[part_of], weights.at[part_of], w_sem.at[i]))

    barrier = pltpu.get_barrier_semaphore()
    line = v // 2
    has_low = line > 0
    has_high = line < n_vocab // 2 - 1
    ends = has_low.astype(jnp.int32) + has_high.astype(jnp.int32)

    def signal(sem, to):
        pl.semaphore_signal(sem, inc=1, device_id=to, device_id_type=MESH)

    def signal_line(sem):
        @pl.when(has_low)
        def _():
            signal(sem, (d, v - 2))

        @pl.when(has_high)
        def _():
            signal(sem, (d, v + 2))

    direct_peers = [to for stage in near for to in stage] + [partner]
    for to in direct_peers:
        signal(barrier, to)
    signal_line(barrier)
    for c in w_copies:
        c.start()
    pl.semaphore_wait(barrier, len(direct_peers) + ends)

    def line_round(k):
        def run():
            signal_line(seen.at[k])
            pl.semaphore_wait(seen.at[k], ends)
        return run

    def peer_round(k, peers):
        def run():
            for to in peers:
                signal(seen.at[k], to)
            pl.semaphore_wait(seen.at[k], len(peers))
        return run

    n_line = n_vocab // 2 - 2
    chores = [line_round(k) for k in range(n_line)]
    for k, peers in enumerate(near + [[partner]]):
        chores.append(peer_round(n_line + k, peers))

    code_copies = []
    for r in range(n_roles):
        to = ((d + 1 + r) % n_dp, v)
        for s, (src, dst) in enumerate(((temp_ref, codes_t), (minp_ref, codes_p))):
            code_copies.append(pltpu.make_async_remote_copy(
                src_ref=src, dst_ref=dst.at[r], send_sem=code_send.at[s, r],
                recv_sem=code_recv.at[s, r], device_id=to, device_id_type=MESH))

    def start_codes():
        for c in code_copies:
            c.start()

    chores.append(start_codes)

    def chore(count=1):
        for _ in range(min(count, len(chores))):
            chores.pop(0)()

    n_units = n_chunks * SPLIT
    width = depth // SPLIT

    def own_piece(u):
        at = pl.multiple_of((u // SPLIT) * chunk_rows + core * PIECE, PIECE)
        return own.at[pl.ds(at, PIECE), pl.ds((u % SPLIT) * width, width)]

    def slot(u, r):
        return gathered.at[u // SPLIT, r, core, :, pl.ds((u % SPLIT) * width, width)]

    def send(src, u, r, sem):
        return pltpu.make_async_remote_copy(
            src_ref=src, dst_ref=slot(u, r), send_sem=sem, recv_sem=ici_recv.at[r, u],
            device_id=targets[r], device_id_type=MESH)

    def to_partner(u, r):
        return pltpu.make_async_remote_copy(
            src_ref=slot(u, r), dst_ref=slot(u, r), send_sem=core_send.at[r, u],
            recv_sem=core_recv.at[r, u], device_id=partner, device_id_type=MESH)

    direct = [0] if relayed else list(range(n_roles))
    others = [r for r in range(n_roles) if r not in direct]
    sends = {}
    for u in range(n_units):
        for r in range(n_roles):
            src = own_piece(u) if r in direct else slot(u, 0)
            sends[r, u] = send(src, u, r, ici_send.at[r, u])
    passes = {(r, u): to_partner(u, r) for r in range(n_roles) for u in range(n_units)}
    own_copy.wait()
    for u in range(n_units):
        for r in direct:
            sends[r, u].start()
    chore(3)

    def take_direct(u):
        for r in direct:
            sends[r, u].wait_recv()
            for o in others:
                sends[o, u].start()
            passes[r, u].start()

    def take_others(u):
        for r in others:
            sends[r, u].wait_recv()
            passes[r, u].start()

    def local_max(values):
        return functools.reduce(jnp.maximum, [values[:, t * LANES:(t + 1) * LANES] for t in range(WIDE // LANES)])

    def to_row(values, op):
        return op(values.T, axis=0, keepdims=True)

    take_direct(0)
    for c in w_copies:
        c.wait()

    def own_step(n, best):
        cols = pl.ds(pl.multiple_of(n * WIDE, WIDE), WIDE)
        out = jnp.dot(own[...], weights[:, cols], preferred_element_type=jnp.float32)
        logits[0, :, cols] = out
        return jnp.maximum(best, local_max(out))

    best = lax.fori_loop(0, vocab // WIDE, own_step, jnp.full((rows, LANES), -jnp.inf, jnp.float32))
    max_box[0, pl.ds(d, 1), :] = to_row(best, jnp.max)

    def column(row):
        return jnp.broadcast_to(row, (LANES, LANES)).T

    def keep_columns(r, temp, minp):
        inv_col[r] = column(1.0 / (temp.astype(jnp.float32) * 0.01))
        base_col[r] = column(1.0 - jnp.log(minp.astype(jnp.float32) * 0.01))

    keep_columns(0, temp_ref[...], minp_ref[...])

    early = max(n_chunks - 2, 1)
    for u in range(1, n_units):
        take_direct(u)
        chore()
        if u <= early * SPLIT:
            take_others(u - 1)
    chore(len(chores))

    for chunks in [range(early)] + [range(i, i + 1) for i in range(early, n_chunks)]:
        g, group = chunks[0], len(chunks)
        if g:
            for u in range(g * SPLIT, (g + 1) * SPLIT):
                take_others(u)
        if g == early:
            for c in code_copies:
                c.wait()
            for r in range(n_roles):
                s = ((d + n_dp - blocks[r]) % n_dp) - 1
                keep_columns(r + 1, codes_t[s], codes_p[s])
        for u in range(g * SPLIT, (g + group) * SPLIT):
            for r in range(n_roles):
                passes[r, u].wait_recv()
        many = group * n_roles * chunk_rows

        def step(n, best):
            cols = pl.ds(pl.multiple_of(n * WIDE, WIDE), WIDE)
            lhs = gathered[g:g + group].reshape(many, depth)
            out = jnp.dot(lhs, weights[:, cols], preferred_element_type=jnp.float32)
            for a, i in enumerate(chunks):
                for r in range(n_roles):
                    at = (a * n_roles + r) * chunk_rows
                    logits[r + 1, i * chunk_rows:(i + 1) * chunk_rows, cols] = out[at:at + chunk_rows]
            return jnp.maximum(best, local_max(out))

        best = lax.fori_loop(0, vocab // WIDE, step, jnp.full((many, LANES), -jnp.inf, jnp.float32))
        for r in range(n_roles):
            rows_r = [best[(a * n_roles + r) * chunk_rows:(a * n_roles + r + 1) * chunk_rows] for a in range(group)]
            piece = jnp.concatenate(rows_r, axis=0)
            max_box[0, pl.ds(blocks[r], 1), g * chunk_rows:(g + group) * chunk_rows] = to_row(piece, jnp.max)

    def exchange(source, box, send_sem, recv_sem):
        def send_row(down, skip):
            to_d = (d + down) % n_dp
            for across in reversed(range(skip, n_vocab)):
                pltpu.make_async_remote_copy(
                    src_ref=source(to_d), dst_ref=box.at[down * n_vocab + across],
                    send_sem=send_sem, recv_sem=recv_sem,
                    device_id=(to_d, (v + across) % n_vocab), device_id_type=MESH).start()

        if n_dp > 4:
            pl.loop(1, n_dp)(lambda down: send_row(down, 0))
        else:
            for down in range(1, n_dp):
                send_row(down, 0)
        send_row(0, 1)

        rest = box.at[pl.ds(1, n_all - 1)]
        return pltpu.make_async_copy(rest, rest, send_sem), pltpu.make_async_copy(rest, rest, recv_sem)

    max_sent, max_got = exchange(lambda block: max_box.at[0], max_box, max_send, max_recv)
    max_got.wait()
    tops[...] = jnp.max(max_box[...], axis=0)
    max_sent.wait()

    lane_tiles = vocab // LANES
    strip = 32
    for r in range(n_dp):
        block = d if r == 0 else blocks[r - 1]
        top_col[...] = column(tops[pl.ds(block, 1), :])

        @pl.loop(0, rows // strip)
        def _(q):
            at = pl.ds(pl.multiple_of(q * strip, strip), strip)
            top, inv, base = top_col[at], inv_col[r, at], base_col[r, at]
            total = count = mass = jnp.zeros((strip, LANES), jnp.float32)
            for t in range(lane_tiles):
                below = (logits[r, at, t * LANES:(t + 1) * LANES] - top) * inv
                term = jnp.exp(below)
                ramp = jnp.clip(below + base, 0.0, 1.0)
                total, count, mass = total + term, count + ramp, mass + ramp * term
            sums[0, at], sums[1, at], sums[2, at] = total, count, mass

        rows_of = [to_row(sums[s], jnp.sum) for s in range(3)]
        part[pl.ds(block, 1)] = jnp.concatenate(rows_of + [jnp.zeros_like(rows_of[0])], axis=0)[None]

    sum_box[0] = part[d]
    sum_sent, sum_got = exchange(lambda block: part.at[block], sum_box, sum_send, sum_recv)
    temperature = temp_ref[...].astype(jnp.float32) * 0.01
    top_score = tops[pl.ds(d, 1), :] / temperature
    sum_got.wait()
    whole = jnp.sum(sum_box[...], axis=0)
    total, count, mass = whole[0:1], whole[1:2], whole[2:3]
    out_ref[0:1] = top_score + jnp.log(total)
    out_ref[1:2] = mass / total
    out_ref[2:3] = jnp.log(1.0 + count)

    sum_sent.wait()
    for c in (*sends.values(), *passes.values()):
        c.wait_send()


def on_device(n_dp, n_vocab, hidden_states, unembed, temp_code, minp_code):
    rows, depth = hidden_states.shape
    vocab = unembed.shape[1]
    n_all = n_dp * n_vocab
    n_roles = n_dp - 1
    n_chunks = rows // (2 * PIECE)
    f32, i32, bf16 = jnp.float32, jnp.int32, hidden_states.dtype
    dma = pltpu.SemaphoreType.DMA
    vmem = pl.BlockSpec(memory_space=pltpu.VMEM)
    any_space = pl.BlockSpec(memory_space=pl.ANY)
    outs = pl.pallas_call(
        functools.partial(kernel, n_dp, n_vocab),
        out_shape=jax.ShapeDtypeStruct((3, rows), f32),
        in_specs=[any_space, any_space, vmem, vmem],
        out_specs=vmem,
        scratch_shapes=[
            pltpu.VMEM((rows, depth), bf16),
            pltpu.VMEM((depth, vocab), bf16),
            pltpu.VMEM((n_chunks, n_roles, 2, PIECE, depth), bf16),
            pltpu.VMEM((n_dp, rows, vocab), f32),
            pltpu.VMEM((n_roles, 1, rows), i32),
            pltpu.VMEM((n_roles, 1, rows), i32),
            pltpu.VMEM((n_dp, rows, LANES), f32),
            pltpu.VMEM((n_dp, rows, LANES), f32),
            pltpu.VMEM((3, rows, LANES), f32),
            pltpu.VMEM((rows, LANES), f32),
            pltpu.VMEM((n_dp, rows), f32),
            pltpu.VMEM((n_all, n_dp, rows), f32),
            pltpu.VMEM((n_dp, 4, rows), f32),
            pltpu.VMEM((n_all, 4, rows), f32),
            dma, dma((4,)),
            *[dma((n_roles, n_chunks * SPLIT))] * 4,
            dma((2, n_roles)), dma((2, n_roles)),
            dma, dma, dma, dma,
            pltpu.SemaphoreType.REGULAR((n_vocab // 2 + 1,)),
        ],
        compiler_params=pltpu.CompilerParams(collective_id=0, has_side_effects=True),
    )(hidden_states, unembed, temp_code.reshape(1, rows), minp_code.reshape(1, rows))
    return outs[0], outs[1], outs[2]


def solution(mesh):
    in_specs = (P("dp", None), P(None, ("dp", "vocab")), P("dp"), P("dp"))
    out_specs = (P("dp"), P("dp"), P("dp"))
    body = functools.partial(on_device, mesh.shape["dp"], mesh.shape["vocab"])
    return jax.shard_map(body, mesh=mesh, in_specs=in_specs, out_specs=out_specs, check_vma=False)
```
